32 devices in a mesh: gx: 4 (over y, core), gy: 8 (over z, x).
Axes of the slice: x: 2, y: 2, z: 4, core: 2. Of those that a mesh axis runs over, the one named last changes fastest.
Arguments:
- offsets: float32 [2, 8, 64, 128], P(None, 'gx', 'gy'), may hold values from 0 to 1
- masses: float32 [8, 64, 128], P('gx', 'gy'), may hold values from 0.01 to 0.04
- counts: int32 [8, 64], P('gx', 'gy'), may hold values from 1 to 128, as said below
- source: float32 [8, 64, 128], P('gx', 'gy'), may hold values from -6 to 6
Outputs:
- density: float32 [8, 64, 128], P('gx', 'gy')
- pressure: float32 [8, 64, 128], P('gx', 'gy')
- residual: float32 [8, 64, 128], P('gx', 'gy')
- peaks: float32 [5], replicated
The draws below stay inside these ranges and needn't reach their ends.
Inputs may be any that keep to these rules, and one draw needn't show every extreme that they name: `counts`: each cell's occupied slots come first; some cell holds 128 particles.
All inputs are finite; a program needn't handle non-finite values.
Results may differ from the reference program's by a relative error of at most 0.0003.
Values sent between devices are 32-bit elements; how exact they have to be, the bound alone decides.
A program may use at most 64 MiB of HBM per device.

```python
import math
import jax
import jax.numpy as jnp
from jax import lax

SLOT = 128
ITERS = 5
NX = 8
NY = 64


def draw_counts(key, part):
    coarse_key = jax.random.fold_in(key, 11)
    fine_key = jax.random.fold_in(key, 12)
    region_rows = (NX + 3) // 4
    region_cols = (NY + 3) // 4
    floor_count = jax.random.randint(coarse_key, (region_rows, region_cols), 1, SLOT + 1)
    floor_count = jnp.repeat(jnp.repeat(floor_count, 4, axis=0), 4, axis=1)[:NX, :NY]
    counts = jax.random.randint(fine_key, (NX, NY), floor_count, SLOT + 1)
    return counts.at[0, 0].set(SLOT).astype(jnp.int32)


def draw_source(key, part):
    rough = jnp.clip(jax.random.normal(jax.random.fold_in(key, 21), (NX, NY, SLOT), jnp.float32), -6.0, 6.0)
    return rough


def level_of(key, dims, cuts, least, top_value):
    def one(dim, parts):
        steps = jax.random.uniform(jax.random.fold_in(jax.random.fold_in(key, 6), dim), (parts,), jnp.float32, least / len(cuts), top_value / len(cuts))
        return jnp.repeat(jnp.exp(steps), dims[dim] // parts).reshape((-1,) + (1,) * (len(dims) - dim - 1))

    level = one(*cuts[0])
    for cut in cuts[1:]:
        level = level * one(*cut)
    return level


def setup_inputs(seed: int = 0) -> dict:
    key_list = jax.random.split(jax.random.key(seed), 5)
    return {
        "offsets": jnp.clip(1.0 * jax.random.uniform(key_list[0], (2, NX, NY, SLOT), jnp.float32) ** level_of(key_list[0], (2, NX, NY, SLOT), ((1, 4), (2, 8)), -0.2, 0.2), 0.0, 1.0),
        "masses": jnp.clip(jnp.exp(math.log(0.04) - 1.3862944 * jax.random.uniform(key_list[1], (NX, NY, SLOT), jnp.float32) ** level_of(key_list[1], (NX, NY, SLOT), ((0, 4), (1, 8)), -0.2, 0.2)), 0.01, 0.04),
        "counts": draw_counts(jax.random.fold_in(key_list[4], 71), 0),
        "source": draw_source(jax.random.fold_in(key_list[4], 71), 0),
    }


BASE_STIFF = 0.5
PAIR_SCALE = 0.05
NEIGHBOUR_STEPS = [(step_x, step_y) for step_x in (-1, 0, 1) for step_y in (-1, 0, 1)]


def near_view(padded, step_x, step_y):
    row_count = padded.shape[-3] - 2
    col_count = padded.shape[-2] - 2
    return padded[..., 1 + step_x:1 + step_x + row_count, 1 + step_y:1 + step_y + col_count, :]


def kernel_terms(own_cells, nearby, step_x, step_y):
    offset_x = (step_x + nearby[0][..., None, :]) - own_cells[0][..., :, None]
    offset_y = (step_y + nearby[1][..., None, :]) - own_cells[1][..., :, None]
    return jnp.maximum(1.0 - (offset_x * offset_x + offset_y * offset_y), 0.0)


def density_block(padded):
    own_cells = near_view(padded, 0, 0)
    summed = jnp.zeros(own_cells.shape[1:], jnp.float32)
    for step_x, step_y in NEIGHBOUR_STEPS:
        nearby = near_view(padded, step_x, step_y)
        falloff = kernel_terms(own_cells, nearby, step_x, step_y)
        summed = summed + jnp.sum(falloff * falloff * falloff * nearby[2][..., None, :], axis=-1)
    return 1.0 + summed


def pair_weights(padded, step_x, step_y):
    own_cells = near_view(padded, 0, 0)
    nearby = near_view(padded, step_x, step_y)
    falloff = kernel_terms(own_cells, nearby, step_x, step_y)
    pairing = own_cells[3][..., :, None] * nearby[3][..., None, :] * (2.0 * PAIR_SCALE) / (own_cells[4][..., :, None] + nearby[4][..., None, :])
    return falloff * falloff * pairing


def diag_block(padded):
    own_cells = near_view(padded, 0, 0)
    summed = jnp.zeros(own_cells.shape[1:], jnp.float32)
    for step_x, step_y in NEIGHBOUR_STEPS:
        summed = summed + jnp.sum(pair_weights(padded, step_x, step_y), axis=-1)
    return BASE_STIFF + summed


def apply_block(padded, padded_field):
    own_cells = near_view(padded, 0, 0)
    summed = jnp.zeros(own_cells.shape[1:], jnp.float32)
    for step_x, step_y in NEIGHBOUR_STEPS:
        summed = summed + jnp.einsum('xyij,xyj->xyi', pair_weights(padded, step_x, step_y), near_view(padded_field, step_x, step_y), precision=lax.Precision.HIGHEST)
    return summed


def reference(offsets, masses, counts, source):
    slot_count = offsets.shape[-1]
    occupied = (jnp.arange(slot_count, dtype=jnp.int32)[None, None, :] < counts[:, :, None]).astype(jnp.float32)
    fields = jnp.stack([offsets[0], offsets[1], masses * occupied, occupied])
    padded = jnp.pad(fields, ((0, 0), (1, 1), (1, 1), (0, 0)))
    row_ids = jnp.arange(fields.shape[1], dtype=jnp.int32)
    density = lax.map(lambda row_index: density_block(lax.dynamic_slice_in_dim(padded, row_index, 3, 1))[0], row_ids)
    full = jnp.concatenate([padded, jnp.pad(density, ((1, 1), (1, 1), (0, 0)))[None]], 0)
    diagonal = lax.map(lambda row_index: diag_block(lax.dynamic_slice_in_dim(full, row_index, 3, 1))[0], row_ids)

    def operate(vector):
        padded_field = jnp.pad(vector, ((1, 1), (1, 1), (0, 0)))
        sums = lax.map(lambda row_index: apply_block(lax.dynamic_slice_in_dim(full, row_index, 3, 1), lax.dynamic_slice_in_dim(padded_field, row_index, 3, 0))[0], row_ids)
        return diagonal * vector - sums

    pressure = jnp.zeros_like(source)
    residual = source * occupied
    scaled = residual / diagonal
    direction = scaled
    precond_now = jnp.sum(residual * scaled)
    peak_list = []
    for step in range(ITERS):
        image = operate(direction)
        step_size = precond_now / jnp.sum(direction * image)
        pressure = pressure + step_size * direction
        residual = residual - step_size * image
        peak_list.append(jnp.max(jnp.abs(residual)))
        scaled = residual / diagonal
        precond_next = jnp.sum(residual * scaled)
        direction = scaled + (precond_next / precond_now) * direction
        precond_now = precond_next
    return density, pressure, residual, jnp.stack(peak_list)
```

```python
import functools

import jax
import jax.numpy as jnp
from jax import lax
from jax.experimental import pallas as pl
from jax.experimental.pallas import tpu as pltpu
from jax.sharding import PartitionSpec as P

ITERS = 5
BASE_STIFF = 0.5
PAIR_SCALE = 0.05
NEIGHBOUR_STEPS = [(step_x, step_y) for step_x in (-1, 0, 1) for step_y in (-1, 0, 1)]
SIDES = [step for step in NEIGHBOUR_STEPS if step != (0, 0)]
MESH = pl.DeviceIdType.MESH
SUMS = 8


def own_edge(step, count):
    return {1: pl.ds(count - 1, 1), -1: pl.ds(0, 1), 0: pl.ds(0, count)}[step]


def halo_edge(step, count):
    return {1: pl.ds(0, 1), -1: pl.ds(count + 1, 1), 0: pl.ds(1, count)}[step]


def inner_edge(step, count):
    return {1: pl.ds(count, 1), -1: pl.ds(1, 1), 0: pl.ds(1, count)}[step]


def kernel(
    size_x, size_y, row_count, col_count,
    fields_ref, rows_ref,
    density_ref, pressure_ref, residual_ref, peaks_ref,
    pad_fields, pad_density, pad_vector, weights, gather_x, gather_y, direction_ref, along_ref,
    field_send, field_recv, density_send, density_recv, vector_send, vector_recv,
    send_x, recv_x, send_y, recv_y,
):
    here_x, here_y = lax.axis_index("gx"), lax.axis_index("gy")
    cell_count = row_count * col_count
    slots = rows_ref.shape[-1]

    for pad in (pad_fields, pad_density):
        pad[...] = jnp.zeros_like(pad)
    for step in range(ITERS):
        pad_vector[step] = jnp.zeros(pad_vector.shape[1:], jnp.float32)

    low_x, high_x = (here_x > 0), (here_x < size_x - 1)
    low_y, high_y = (here_y > 0), (here_y < size_y - 1)

    def there(step, low, high):
        return {1: high, -1: low}[step]

    def on_side(step_x, step_y, action):
        conditions = []
        if step_x:
            conditions.append(there(step_x, low_x, high_x))
        if step_y:
            conditions.append(there(step_y, low_y, high_y))
        condition = conditions[0]
        for other in conditions[1:]:
            condition = jnp.logical_and(condition, other)
        pl.when(condition)(action)

    barrier = pltpu.get_barrier_semaphore()

    def greet(device):
        pl.semaphore_signal(barrier, inc=1, device_id=device, device_id_type=MESH)

    for ahead in range(1, size_x):
        greet((lax.rem(here_x + ahead, size_x), here_y))
    for ahead in range(1, size_y):
        greet((here_x, lax.rem(here_y + ahead, size_y)))
    for step_x, step_y in SIDES:
        if step_x and step_y:
            on_side(step_x, step_y, functools.partial(greet, (here_x + step_x, here_y + step_y)))
    as_int = lambda flag: flag.astype(jnp.int32)
    corners = (as_int(low_x) + as_int(high_x)) * (as_int(low_y) + as_int(high_y))
    pl.semaphore_wait(barrier, size_x - 1 + size_y - 1 + corners)

    def halo_copy(side, source_of, target, send_sem, recv_sem):
        step_x, step_y = SIDES[side]
        return pltpu.make_async_remote_copy(
            src_ref=source_of(step_x, step_y),
            dst_ref=target.at[halo_edge(step_x, row_count), halo_edge(step_y, col_count)],
            send_sem=send_sem.at[side],
            recv_sem=recv_sem.at[side],
            device_id=(here_x + step_x, here_y + step_y),
            device_id_type=MESH,
        )

    def inner_of(pad):
        return lambda step_x, step_y: pad.at[
            inner_edge(step_x, row_count), inner_edge(step_y, col_count)
        ]

    def start_exchange(*args):
        for side, (step_x, step_y) in enumerate(SIDES):
            on_side(step_x, step_y, lambda side=side: halo_copy(side, *args).start())

    def end_exchange(*args):
        for side, (step_x, step_y) in enumerate(SIDES):
            on_side(-step_x, -step_y, lambda side=side: halo_copy(side, *args).wait_recv())
        for side, (step_x, step_y) in enumerate(SIDES):
            on_side(step_x, step_y, lambda side=side: halo_copy(side, *args).wait_send())

    lanes = lax.broadcasted_iota(jnp.int32, (slots, slots), 1)

    def as_columns(rows):
        filler = jnp.zeros((slots - cell_count, slots), jnp.float32)
        return jnp.concatenate([rows, filler], axis=0).T

    def as_rows(columns):
        return columns.T[:cell_count]

    def column(columns, cell):
        return jnp.sum(jnp.where(lanes == cell, columns, 0.0), axis=1, keepdims=True)

    def over_cells(terms):
        def one(cell, columns):
            total = terms(cell, lax.div(cell, col_count) + 1, lax.rem(cell, col_count) + 1)
            return jnp.where(lanes == cell, jnp.sum(total, axis=1, keepdims=True), columns)

        return lax.fori_loop(0, cell_count, one, jnp.zeros((slots, slots), jnp.float32))

    def put_rows(rows, pad):
        for cell in range(cell_count):
            pad[cell // col_count + 1, cell % col_count + 1] = rows[cell : cell + 1]

    field_args = (
        lambda step_x, step_y: fields_ref.at[
            own_edge(step_x, row_count), own_edge(step_y, col_count)
        ],
        pad_fields, field_send, field_recv,
    )
    start_exchange(*field_args)
    pad_fields[pl.ds(1, row_count), pl.ds(1, col_count)] = fields_ref[...]
    columns_x, columns_y = as_columns(rows_ref[0]), as_columns(rows_ref[1])
    occupied = rows_ref[2]
    end_exchange(*field_args)

    def density_terms(cell, at_x, at_y):
        own_x, own_y = column(columns_x, cell), column(columns_y, cell)
        total = jnp.zeros((slots, slots), jnp.float32)
        for index, (step_x, step_y) in enumerate(NEIGHBOUR_STEPS):
            near = pad_fields[at_x + step_x, at_y + step_y]
            offset_x = (step_x + near[0:1]) - own_x
            offset_y = (step_y + near[1:2]) - own_y
            falloff = jnp.maximum(1.0 - (offset_x * offset_x + offset_y * offset_y), 0.0)
            square = falloff * falloff
            weights[cell, index] = square
            total = total + square * falloff * near[2:3]
        return total

    density = 1.0 + as_rows(over_cells(density_terms))
    density_ref[...] = density
    put_rows(density, pad_density)

    density_args = (inner_of(pad_density), pad_density, density_send, density_recv)
    start_exchange(*density_args)
    columns_density = as_columns(density)
    end_exchange(*density_args)

    def weight_terms(cell, at_x, at_y):
        own_density = column(columns_density, cell)
        total = jnp.zeros((slots, slots), jnp.float32)
        for index, (step_x, step_y) in enumerate(NEIGHBOUR_STEPS):
            near = pad_fields[at_x + step_x, at_y + step_y]
            near_density = pad_density[at_x + step_x, at_y + step_y]
            weight = weights[cell, index] * ((2.0 * PAIR_SCALE) / (own_density + near_density))
            weights[cell, index] = weight
            total = total + weight * near[3:4]
        return total

    diagonal = BASE_STIFF + occupied * as_rows(over_cells(weight_terms))

    message_row = lax.broadcasted_iota(jnp.int32, (SUMS, slots), 0)

    def spread(parts, index, size, here, gather, send_sem, recv_sem, axis):
        slot = gather.at[index]
        slot[here] = parts

        def copy(ahead, owner):
            peer = lax.rem(here + ahead, size)
            return pltpu.make_async_remote_copy(
                src_ref=slot.at[here],
                dst_ref=slot.at[owner(peer)],
                send_sem=send_sem.at[ahead],
                recv_sem=recv_sem.at[index, owner(peer)],
                device_id=(peer, here_y) if axis == 0 else (here_x, peer),
                device_id_type=MESH,
            )

        for ahead in range(1, size):
            copy(ahead, lambda peer: here).start()
        for ahead in range(1, size):
            copy(ahead, lambda peer: peer).wait_recv()
        for ahead in range(1, size):
            copy(ahead, lambda peer: here).wait_send()
        summed = largest = slot[0]
        for other in range(1, size):
            summed = summed + slot[other]
            largest = jnp.maximum(largest, slot[other])
        return jnp.where(message_row == 2, largest, summed)

    def reduced(index, first, second, magnitude):
        total = lambda rows: jnp.sum(rows, axis=0, keepdims=True)
        peak = jnp.max(magnitude, axis=0, keepdims=True)
        parts = jnp.where(
            message_row == 0,
            total(first),
            jnp.where(message_row == 1, total(second), jnp.where(message_row == 2, peak, 0.0)),
        )
        parts = spread(parts, index, size_x, here_x, gather_x, send_x, recv_x, 0)
        parts = spread(parts, index, size_y, here_y, gather_y, send_y, recv_y, 1)
        sums = jnp.sum(parts, axis=1, keepdims=True)
        peaks = jnp.max(parts, axis=1, keepdims=True)
        wide = lambda one: jnp.broadcast_to(one, (1, slots))
        return wide(sums[0:1]), wide(sums[1:2]), wide(peaks[2:3])

    pressure_ref[...] = jnp.zeros_like(pressure_ref)
    residual_ref[...] = rows_ref[3] * occupied
    direction_ref[...] = jnp.zeros_like(direction_ref)
    along_ref[...] = jnp.zeros_like(along_ref)
    peaks_ref[...] = jnp.zeros_like(peaks_ref)

    def iteration(step, carry):
        precond_now, step_size = carry
        residual = residual_ref[...]
        scaled = residual / diagonal
        pad = pad_vector.at[step]
        put_rows(scaled, pad)
        args = (inner_of(pad), pad, vector_send, vector_recv.at[step])
        start_exchange(*args)
        end_exchange(*args)

        def vector_terms(cell, at_x, at_y):
            total = jnp.zeros((slots, slots), jnp.float32)
            for index, (step_x, step_y) in enumerate(NEIGHBOUR_STEPS):
                total = total + weights[cell, index] * pad[at_x + step_x, at_y + step_y]
            return total

        image = diagonal * scaled - occupied * as_rows(over_cells(vector_terms))
        precond_next, curvature, peak = reduced(
            step, residual * scaled, scaled * image, jnp.abs(residual)
        )
        peaks_ref[pl.ds(step, 1)] = peak
        ratio = jnp.where(step == 0, 0.0, precond_next / precond_now)
        step_size = precond_next / (curvature - ratio * precond_next / step_size)
        direction = scaled + ratio * direction_ref[...]
        along = image + ratio * along_ref[...]
        direction_ref[...] = direction
        along_ref[...] = along
        pressure_ref[...] = pressure_ref[...] + step_size * direction
        residual_ref[...] = residual - step_size * along
        return precond_next, step_size

    ones = jnp.ones((1, slots), jnp.float32)
    lax.fori_loop(0, ITERS, iteration, (ones, ones))
    magnitude = jnp.abs(residual_ref[...])
    peaks_ref[pl.ds(ITERS, 1)] = reduced(ITERS, magnitude, magnitude, magnitude)[2]


def body(size_x, size_y, offsets, masses, counts, source):
    row_count, col_count, slots = masses.shape
    cell_count = row_count * col_count
    occupied = (jnp.arange(slots, dtype=jnp.int32)[None, None, :] < counts[:, :, None]).astype(
        jnp.float32
    )
    fields = jnp.stack([offsets[0], offsets[1], masses * occupied, occupied], axis=2)
    rows = jnp.stack([offsets[0], offsets[1], occupied, source]).reshape(4, cell_count, slots)
    padded = (row_count + 2, col_count + 2)
    dma, f32, sides = pltpu.SemaphoreType.DMA, jnp.float32, len(SIDES)
    vmem = pl.BlockSpec(memory_space=pltpu.VMEM)
    block = jax.ShapeDtypeStruct((cell_count, slots), f32)
    density, pressure, residual, peaks = pl.pallas_call(
        functools.partial(kernel, size_x, size_y, row_count, col_count),
        out_shape=(block, block, block, jax.ShapeDtypeStruct((8, slots), f32)),
        in_specs=[vmem] * 2,
        out_specs=(vmem,) * 4,
        scratch_shapes=[
            pltpu.VMEM(padded + (4, slots), f32),
            pltpu.VMEM(padded + (1, slots), f32),
            pltpu.VMEM((ITERS,) + padded + (1, slots), f32),
            pltpu.VMEM((cell_count, len(NEIGHBOUR_STEPS), slots, slots), f32),
            pltpu.VMEM((ITERS + 1, size_x, SUMS, slots), f32),
            pltpu.VMEM((ITERS + 1, size_y, SUMS, slots), f32),
            pltpu.VMEM((cell_count, slots), f32),
            pltpu.VMEM((cell_count, slots), f32),
            dma((sides,)), dma((sides,)),
            dma((sides,)), dma((sides,)),
            dma((sides,)), dma((ITERS, sides)),
            dma((size_x,)), dma((ITERS + 1, size_x)),
            dma((size_y,)), dma((ITERS + 1, size_y)),
        ],
        compiler_params=pltpu.CompilerParams(collective_id=0, has_side_effects=True),
    )(fields, rows)
    shape = (row_count, col_count, slots)
    return (
        density.reshape(shape),
        pressure.reshape(shape),
        residual.reshape(shape),
        peaks[1 : ITERS + 1, 0],
    )


def solution(mesh):
    in_specs = (P(None, "gx", "gy", None), P("gx", "gy", None), P("gx", "gy"), P("gx", "gy", None))
    out_specs = (P("gx", "gy", None), P("gx", "gy", None), P("gx", "gy", None), P())
    return jax.shard_map(
        functools.partial(body, mesh.shape["gx"], mesh.shape["gy"]),
        mesh=mesh, in_specs=in_specs, out_specs=out_specs, check_vma=False,
    )
```
